128 devices in a mesh: lat: 32 (over z, x, core), lev: 4 (over y).
Axes of the slice: x: 4, y: 4, z: 4, core: 2. Of those that a mesh axis runs over, the one named last changes fastest.
Arguments:
- grid: bfloat16 [640, 128, 4, 1280], P('lat', 'lev'), may hold values from -6 to 6
- legendre: bfloat16 [640, 640, 640], P('lat'), may hold values from -0.25 to 0.25
- vertical: bfloat16 [128, 128], P('lev'), may hold values from -0.5 to 0.5
- damping: bfloat16 [128], P('lev'), may hold values from 1 to 16
- lon_counts: int32 [640], replicated, may hold values from 160 to 1280
- wave_slots: int32 [640], replicated, may hold values from 0 to 639, as said below
Outputs:
- filtered_grid: bfloat16 [640, 128, 4, 1280], P('lat', 'lev')
The draws below stay inside these ranges and needn't reach their ends.
Inputs may be any that keep to these rules, and one draw needn't show every extreme that they name: wave_slots is a permutation; slot g * 5 + r holds a wavenumber from r * 128 to (r + 1) * 128 - 1.
All inputs are finite; a program needn't handle non-finite values.
Results may differ from the reference program's by a relative error of at most 0.0074.
Values may be sent and summed in bfloat16 or wider, within the bound.
A program may use at most 128 MiB of HBM per device.

```python
import math
import jax
import jax.numpy as jnp
from jax import lax

NLAT = 640
NLON = 1280
M = 640
FIELDS = 4
LEV = 128
GROUPS = 128
ROUNDS = 5


def draw_wave_slots(key, part):
    keys = jax.random.split(jax.random.fold_in(key, 11), ROUNDS)
    orders = jax.vmap(lambda single: jax.random.permutation(single, GROUPS))(keys)
    base = jnp.arange(ROUNDS, dtype=jnp.int32)[:, None] * GROUPS
    return (base + orders.astype(jnp.int32)).T.reshape(M).astype(jnp.int32)


def place_ends(drawn, rng, smallest, top_value):
    index_at = [jax.random.randint(jax.random.fold_in(rng, axis), (), 0, length) for axis, length in enumerate(drawn.shape)]
    main_axis = drawn.shape.index(max(drawn.shape))
    neighbour = index_at[:main_axis] + [(index_at[main_axis] + 1) % drawn.shape[main_axis]] + index_at[main_axis + 1:]
    return drawn.at[tuple(index_at)].set(smallest).at[tuple(neighbour)].set(top_value)


def block_levels(key, dims, cuts, least, largest):
    def one(dim, blocks):
        steps = jax.random.uniform(jax.random.fold_in(jax.random.fold_in(key, 6), dim), (blocks,), jnp.float32, least / len(cuts), largest / len(cuts))
        return jnp.repeat(jnp.exp(steps), dims[dim] // blocks).reshape((-1,) + (1,) * (len(dims) - dim - 1))

    loudness = one(*cuts[0])
    for cut in cuts[1:]:
        loudness = loudness * one(*cut)
    return loudness


def centred(rng, extent, scale, bound, pieces=(), kind=jnp.bfloat16):
    result = scale * jax.random.normal(rng, extent, jnp.float32)
    if pieces:
        result = result * block_levels(rng, extent, pieces, -0.22, 0.18)
    return jnp.clip(result, -bound, bound).astype(kind)


def setup_inputs(seed: int = 0) -> dict:
    splits = jax.random.split(jax.random.key(seed), 7)
    return {
        "grid": centred(splits[0], (NLAT, LEV, FIELDS, NLON), 1.0, 6.0, ((0, 32), (1, 4))),
        "legendre": centred(splits[1], (M, M, NLAT), NLAT ** -0.5, 0.25, ((0, 32),)),
        "vertical": centred(splits[2], (LEV, LEV), LEV ** -0.5, 0.5, ((0, 4),)),
        "damping": jnp.clip(jnp.exp(math.log(16.0) - 2.7725887 * jax.random.uniform(splits[3], (LEV,), jnp.float32) ** block_levels(splits[3], (LEV,), ((0, 4),), -0.2, 0.2)), 1.0, 16.0).astype(jnp.bfloat16),
        "lon_counts": place_ends(jax.random.randint(splits[4], (NLAT,), NLON // 8, NLON + 1), jax.random.fold_in(splits[4], 1), NLON // 8, NLON).astype(jnp.int32),
        "wave_slots": draw_wave_slots(jax.random.fold_in(splits[6], 71), 0),
    }


def fourier_tables(wavenumbers, longitudes):
    wavenumbers = wavenumbers.astype(jnp.int32)
    points = jnp.arange(longitudes, dtype=jnp.int32)
    phase = (wavenumbers[:, None] * points[None, :] % longitudes).astype(jnp.float32) * (2.0 * math.pi / longitudes)
    scale = 1.0 / math.sqrt(longitudes)
    cosine = jnp.cos(phase) * scale
    sine = jnp.sin(phase) * scale
    forward_table = jnp.stack([cosine, -sine], axis=1).astype(jnp.bfloat16)
    weight = jnp.where(wavenumbers == 0, 1.0, 2.0).astype(jnp.float32)[:, None]
    inverse_table = jnp.stack([cosine * weight, -sine * weight], axis=1).astype(jnp.bfloat16)
    return (forward_table, inverse_table)

def damping_factor(degrees, damping):
    degree_values = jnp.arange(degrees).astype(jnp.float32)
    ratio = degree_values * (degree_values + 1.0) / float(degrees * (degrees - 1))
    return 1.0 / (1.0 + damping.astype(jnp.float32)[None, :] * (ratio * ratio)[:, None])

def reference(grid, legendre, vertical, damping, lon_counts, wave_slots):
    latitudes, levels, fields, longitudes = grid.shape
    wavenumbers = wave_slots.astype(jnp.int32)
    slot_count = wavenumbers.shape[0]
    degrees = legendre.shape[1]
    pair_width = 2 * fields
    forward_table, inverse_table = fourier_tables(wavenumbers, longitudes)
    kept = (2 * wavenumbers[:, None] < lon_counts.astype(jnp.int32)[None, :]).astype(jnp.float32)
    fourier = jnp.einsum('mrx,alfx->mlrfa', forward_table.astype(jnp.float32), grid.astype(jnp.float32))
    fourier = (fourier * kept[:, None, None, None, :]).astype(jnp.bfloat16)
    fourier = fourier.reshape(slot_count, levels * pair_width, latitudes)
    factor = damping_factor(degrees, damping)
    mixer = vertical.astype(jnp.float32)

    def one_slot(item):
        table, block, wave = item
        spectral = jnp.dot(table, block.T, preferred_element_type=jnp.float32)
        live = (jnp.arange(degrees, dtype=jnp.int32) >= wave).astype(jnp.float32)
        spectral = (spectral * live[:, None]).astype(jnp.bfloat16).reshape(degrees, levels, pair_width)
        stacked = spectral.astype(jnp.float32)
        mixed = (stacked + jnp.einsum('nkc,lk->nlc', stacked, mixer)) * factor[:, :, None]
        mixed = mixed.astype(jnp.bfloat16).reshape(degrees, levels * pair_width)
        banded = jnp.dot(mixed.T, table, preferred_element_type=jnp.float32)
        return banded.astype(jnp.bfloat16)
    banded = lax.map(one_slot, (legendre, fourier, wavenumbers))
    banded = banded.reshape(slot_count, levels, 2, fields, latitudes).astype(jnp.float32) * kept[:, None, None, None, :]
    filtered_grid = jnp.einsum('mlrfa,mrx->alfx', banded, inverse_table.astype(jnp.float32))
    return filtered_grid.astype(jnp.bfloat16)
```

```python
import functools
import math

import jax
import jax.numpy as jnp
from jax import lax
from jax.experimental import pallas as pl
from jax.experimental.pallas import tpu as pltpu
from jax.sharding import PartitionSpec as P


def sent_together(arrays, axis, dim, along):
    widths = [math.prod(a.shape[along:]) for a in arrays]
    both = jnp.concatenate(
        [a.reshape(*a.shape[:along], w) for a, w in zip(arrays, widths)], axis=along
    )
    result = lax.all_gather(both, axis, axis=dim, tiled=True)
    pieces = jnp.split(result, [sum(widths[:k]) for k in range(1, len(widths))], axis=along)
    return tuple(
        (b.reshape(*result.shape[:along], *a.shape[along:]) for a, b in zip(arrays, pieces))
    )


def exchange_kernel(rounds, x_ref, o_ref, send_sem, recv_sem):
    i = lax.axis_index("lat")
    j = lax.axis_index("lev")
    me = i * 4 + j
    z, x, c = i // 8, (i // 2) % 4, i % 2

    def partner(k):
        q = (k * 45) % 128
        dy, dc, dx, dz = q % 4, (q // 4) % 2, (q // 8) % 4, q // 32
        i2 = (((z + dz) % 4) * 4 + (x + dx) % 4) * 2 + (c + dc) % 2
        return i2, (j + dy) % 4

    barrier = pltpu.get_barrier_semaphore()

    def greet(k, carry):
        pl.semaphore_signal(
            barrier, inc=1, device_id=partner(k), device_id_type=pl.DeviceIdType.MESH
        )
        return carry

    lax.fori_loop(1, 128, greet, 0)
    pl.semaphore_wait(barrier, 127)
    for r in range(rounds):

        def send(k, carry, r=r):
            i2, j2 = partner(k)
            pltpu.make_async_remote_copy(
                src_ref=x_ref.at[r, i2 * 4 + j2],
                dst_ref=o_ref.at[r, me],
                send_sem=send_sem.at[r],
                recv_sem=recv_sem.at[r],
                device_id=(i2, j2),
                device_id_type=pl.DeviceIdType.MESH,
            ).start()
            return carry

        lax.fori_loop(1, 128, send, 0)
    o_ref[:, me] = x_ref[:, me]
    for r in range(rounds):
        pltpu.make_async_copy(
            x_ref.at[r, pl.ds(0, 127)], x_ref.at[r, pl.ds(0, 127)], send_sem.at[r]
        ).wait()
        pltpu.make_async_copy(
            o_ref.at[r, pl.ds(0, 127)], o_ref.at[r, pl.ds(0, 127)], recv_sem.at[r]
        ).wait()


def exchange(x, collective_id):
    rounds = x.shape[0]
    return pl.pallas_call(
        functools.partial(exchange_kernel, rounds),
        out_shape=jax.ShapeDtypeStruct(x.shape, x.dtype),
        in_specs=[pl.BlockSpec(memory_space=pltpu.VMEM)],
        out_specs=pl.BlockSpec(memory_space=pltpu.VMEM),
        scratch_shapes=[
            pltpu.SemaphoreType.DMA((rounds,)),
            pltpu.SemaphoreType.DMA((rounds,)),
        ],
        compiler_params=pltpu.CompilerParams(
            collective_id=collective_id, has_side_effects=True, vmem_limit_bytes=40 * 2**20
        ),
    )(x)


def forward_build(wavenumbers, longitudes):
    points = jnp.arange(longitudes, dtype=jnp.int32)
    phase = (wavenumbers[:, None] * points[None, :] % longitudes).astype(jnp.float32) * (
        2.0 * math.pi / longitudes
    )
    scale = 1.0 / math.sqrt(longitudes)
    return jnp.stack([jnp.cos(phase) * scale, -jnp.sin(phase) * scale], axis=1).astype(jnp.bfloat16)


def inverse_build(wavenumbers, longitudes):
    points = jnp.arange(longitudes, dtype=jnp.int32)
    phase = (wavenumbers[:, None] * points[None, :] % longitudes).astype(jnp.float32) * (
        2.0 * math.pi / longitudes
    )
    scale = 1.0 / math.sqrt(longitudes)
    weight = jnp.where(wavenumbers == 0, 1.0, 2.0).astype(jnp.float32)[:, None]
    return jnp.stack(
        [jnp.cos(phase) * scale * weight, -jnp.sin(phase) * scale * weight], axis=1
    ).astype(jnp.bfloat16)


def damping_factor(degrees, damping):
    degree_values = jnp.arange(degrees).astype(jnp.float32)
    ratio = degree_values * (degree_values + 1.0) / float(degrees * (degrees - 1))
    return 1.0 / (1.0 + damping.astype(jnp.float32)[None, :] * (ratio * ratio)[:, None])


def legendre_forward(table, fourier, wavenumbers):
    degrees = table.shape[1]
    spectral = jnp.einsum("sna,srac->snrc", table, fourier, preferred_element_type=jnp.float32)
    live = (jnp.arange(degrees, dtype=jnp.int32)[None, :] >= wavenumbers[:, None]).astype(
        jnp.float32
    )
    return (spectral * live[:, :, None, None]).astype(jnp.bfloat16)


def legendre_inverse(table, mixed):
    banded = jnp.einsum("sna,snrc->srac", table, mixed, preferred_element_type=jnp.float32)
    return banded.astype(jnp.bfloat16)


def per_device(grid, legendre, vertical, damping, lon_counts, wave_slots):
    lat_rows, level_rows, fields, longitudes = grid.shape
    slot_count = wave_slots.shape[0]
    degrees = legendre.shape[1]
    own_slots = legendre.shape[0]
    forward_table = forward_build(wave_slots, longitudes)
    own_counts = lax.dynamic_slice_in_dim(lon_counts, lax.axis_index("lat") * lat_rows, lat_rows)
    fourier = jnp.einsum(
        "mrx,acx->mrac",
        forward_table,
        grid.reshape(lat_rows, level_rows * fields, longitudes),
        preferred_element_type=jnp.float32,
    )
    forward_kept = (2 * wave_slots[:, None] < own_counts[None, :]).astype(jnp.float32)
    fourier = (fourier * forward_kept[:, None, :, None]).astype(jnp.bfloat16)
    blocks = fourier.reshape(128, 5, 2 * lat_rows, level_rows * fields).transpose(1, 0, 2, 3)
    got = exchange(blocks, 0).reshape(5, 32, 4, 2, lat_rows, level_rows * fields)
    gathered = got.transpose(0, 3, 1, 4, 2, 5).reshape(
        5, 2, 32 * lat_rows, 4 * level_rows * fields
    )
    count = gathered.shape[0]
    own_table = lax.dynamic_slice_in_dim(legendre, lax.axis_index("lev") * count, count, 0)
    own_waves = lax.dynamic_slice_in_dim(
        wave_slots, lax.axis_index("lat") * own_slots + lax.axis_index("lev") * count, count
    )
    spectral = legendre_forward(own_table, gathered, own_waves)
    all_rows, all_damping = sent_together((vertical, damping), "lev", 0, 1)
    levels = all_rows.shape[0]
    stacked = spectral.reshape(count, degrees, 2, levels, fields)
    mixed = stacked.astype(jnp.float32) + jnp.einsum(
        "snrkf,lk->snrlf", stacked, all_rows, preferred_element_type=jnp.float32
    )
    mixed = mixed * damping_factor(degrees, all_damping)[None, :, None, :, None]
    mixed = mixed.astype(jnp.bfloat16).reshape(count, degrees, 2, levels * fields)
    banded = legendre_inverse(own_table, mixed)
    back = banded.reshape(5, 2, 32, lat_rows, 4, level_rows * fields).transpose(0, 2, 4, 1, 3, 5)
    back = exchange(back.reshape(5, 128, 2 * lat_rows, level_rows * fields), 1)
    returned = back.reshape(5 * 128, 2, lat_rows, level_rows * fields)
    back_order = wave_slots.reshape(128, 5).transpose(1, 0).reshape(slot_count)
    inverse_table = inverse_build(back_order, longitudes)
    back_kept = (2 * back_order[:, None] < own_counts[None, :]).astype(jnp.bfloat16)
    returned = returned * back_kept[:, None, :, None]
    filtered_grid = jnp.einsum(
        "mrac,mrx->acx", returned, inverse_table, preferred_element_type=jnp.float32
    )
    return filtered_grid.reshape(lat_rows, level_rows, fields, longitudes).astype(jnp.bfloat16)


def solution(mesh):
    return jax.shard_map(
        per_device,
        mesh=mesh,
        in_specs=(
            P("lat", "lev", None, None),
            P("lat", None, None),
            P("lev", None),
            P("lev"),
            P(),
            P(),
        ),
        out_specs=P("lat", "lev", None, None),
        check_vma=False,
    )
```

```python
import functools
import math

import jax
import jax.numpy as jnp
from jax import lax
from jax.experimental import pallas as pl
from jax.experimental.pallas import tpu as pltpu
from jax.sharding import PartitionSpec as P

LAT, LEV = 32, 4
PEERS = LAT * LEV
ROUNDS = 5
ROWS = 20
LANES = 128
LONS = 1280
DEGREES = 640
BF16, F32 = jnp.bfloat16, jnp.float32
MESH = pl.DeviceIdType.MESH
NT = (((1,), (1,)), ((), ()))
TN = (((0,), (0,)), ((), ()))


def step_kernel(
    grid_ref, leg_ref, vd_ref, trig_ref, lon_ref, wave_ref,
    brecv, tab_out,
    gv, legv, tab, fsend, frecv, bsend, vdx, vfull, mixer, factor,
    pair32, half32, xr, legm, mixed,
    grid_sem, leg_sem, tab_sem, vsend_sem, vrecv_sem,
    fsend_sem, frecv_sem, bsend_sem, brecv_sem, own_sem,
):
    i = lax.axis_index("lat")
    j = lax.axis_index("lev")
    me = i * LEV + j
    z, x, c = i // 8, (i // 2) % 4, i % 2

    def partner(k):
        q = (k * 45) % PEERS
        dy, dc, dx, dz = q % 4, (q // 4) % 2, (q // 8) % 4, q // 32
        i2 = (((z + dz) % 4) * 4 + (x + dx) % 4) * 2 + (c + dc) % 2
        return i2, (j + dy) % LEV

    def grid_copy(a):
        return pltpu.make_async_copy(
            grid_ref.at[a].reshape(LANES, LONS), gv.at[a], grid_sem.at[a]
        )

    def leg_copy(r):
        return pltpu.make_async_copy(leg_ref.at[j * ROUNDS + r], legv.at[r], leg_sem.at[r])

    def start_grid(a, carry):
        grid_copy(a).start()
        return carry

    lax.fori_loop(0, ROWS, start_grid, 0)
    for r in range(ROUNDS):
        leg_copy(r).start()

    barrier = pltpu.get_barrier_semaphore()

    def greet(k, carry):
        pl.semaphore_signal(barrier, inc=1, device_id=partner(k), device_id_type=MESH)
        return carry

    lax.fori_loop(1, PEERS, greet, 0)

    def table(r):
        cb = trig_ref[0, r, :, 0:128]
        sb = trig_ref[1, r, :, 0:128]
        for q in range(LONS // 128):
            ca = trig_ref[0, r, :, 128 + q : 129 + q]
            sa = trig_ref[1, r, :, 128 + q : 129 + q]
            half32[pl.ds(0, 128, 2), :] = ca * cb - sa * sb
            half32[pl.ds(1, 128, 2), :] = -(sa * cb + ca * sb)
            tab[r, :, q * 128 : (q + 1) * 128] = half32[...].astype(BF16)
        pltpu.make_async_copy(tab.at[r], tab_out.at[r], tab_sem.at[r]).start()

    def forward(r):
        def pair(p, carry):
            if r == 0:
                grid_copy(2 * p).wait()
                grid_copy(2 * p + 1).wait()
            rows = gv.reshape(ROWS * LANES, LONS)[pl.ds(pl.multiple_of(p * 256, 256), 256), :]
            out = lax.dot_general(tab[r], rows, NT, preferred_element_type=F32).astype(BF16)
            fsend.at[r, 2 * p].reshape(256, 128)[...] = out[:, 0:128]
            fsend.at[r, 2 * p + 1].reshape(256, 128)[...] = out[:, 128:256]
            return carry

        lax.fori_loop(0, ROWS // 2, pair, 0)

    def send_forward(r):
        def send(k, carry):
            i2, j2 = partner(k)
            pltpu.make_async_remote_copy(
                src_ref=fsend.at[r, :, i2 * LEV + j2],
                dst_ref=frecv.at[r, j, pl.ds(i * ROWS, ROWS)],
                send_sem=fsend_sem.at[r],
                recv_sem=frecv_sem.at[r],
                device_id=(i2, j2),
                device_id_type=MESH,
            ).start()
            return carry

        lax.fori_loop(1, PEERS, send, 0)
        frecv[r, j, pl.ds(i * ROWS, ROWS)] = fsend[r, :, me]

    def send_back(r):
        def send(k, carry):
            i2, j2 = partner(k)
            pltpu.make_async_remote_copy(
                src_ref=bsend.at[r, j2, pl.ds(i2 * ROWS, ROWS)],
                dst_ref=brecv.at[r, :, me],
                send_sem=bsend_sem.at[r],
                recv_sem=brecv_sem.at[r],
                device_id=(i2, j2),
                device_id_type=MESH,
            ).start()
            return carry

        lax.fori_loop(1, PEERS, send, 0)
        pltpu.make_async_copy(
            bsend.at[r, j, pl.ds(i * ROWS, ROWS)], brecv.at[r, :, me], own_sem.at[r]
        ).start()

    def wait_bytes(ref, r, sem):
        most = ref.at[r].reshape(ROWS * PEERS, 2, LANES).at[pl.ds(0, ROWS * (PEERS - 1))]
        pltpu.make_async_copy(most, most, sem.at[r]).wait()

    def vertical_copy(d):
        return pltpu.make_async_remote_copy(
            src_ref=vd_ref,
            dst_ref=vdx.at[j],
            send_sem=vsend_sem,
            recv_sem=vrecv_sem,
            device_id=(i, (j + d) % LEV),
            device_id_type=MESH,
        )

    def build_mixer():
        three = vdx.at[pl.ds(0, LEV - 1)]
        pltpu.make_async_copy(three, three, vrecv_sem).wait()
        pltpu.make_async_copy(three, three, vsend_sem).wait()
        for p in range(LEV):
            vfull[p * 32 : (p + 1) * 32, :] = vdx[p, 0:32, :]
        row = lax.broadcasted_iota(jnp.int32, (512, 128), 0)
        col = lax.broadcasted_iota(jnp.int32, (512, 128), 1)
        pick = jnp.where(row // 4 == col, 1.0, 0.0).astype(BF16)
        tall = lax.dot_general(pick, vfull[...], NT, preferred_element_type=F32).astype(BF16)
        wide = lax.dot_general(tall, pick, NT, preferred_element_type=F32)
        row = lax.broadcasted_iota(jnp.int32, (512, 512), 0)
        col = lax.broadcasted_iota(jnp.int32, (512, 512), 1)
        mixer[...] = jnp.where(row % 4 == col % 4, wide, 0.0).astype(BF16)
        damp = vdx[0, 32:48, :].astype(F32)
        for p in range(1, LEV):
            damp = damp + vdx[p, 32:48, :].astype(F32)
        damp = lax.dot_general(damp.astype(BF16), pick, NT, preferred_element_type=F32)[0:1, :]
        for t in range(ROUNDS):
            n = (lax.broadcasted_iota(jnp.int32, (128, 512), 0) + 128 * t).astype(F32)
            ratio = n * (n + 1.0) / float(DEGREES * (DEGREES - 1))
            factor[t * 128 : (t + 1) * 128, :] = 1.0 / (1.0 + damp * (ratio * ratio))

    def spectral(r):
        wave = wave_ref[me * ROUNDS + r]
        weight = jnp.where(wave == 0, 1.0, 2.0).astype(F32)
        for p in range(LEV):
            pair32[...] = frecv.at[r, p].reshape(2 * DEGREES, 128)[...].astype(F32)
            for h in range(2):
                xr[:, h * 512 + p * 128 : h * 512 + (p + 1) * 128] = pair32[
                    pl.ds(h, DEGREES, 2), :
                ].astype(BF16)
        keep = jnp.where(2 * wave < lon_ref[...], 1.0, 0.0)
        for t in range(r, ROUNDS):
            n = lax.broadcasted_iota(jnp.int32, (128, DEGREES), 0) + 128 * t
            tile = jnp.where(n >= wave, legv[r, t * 128 : (t + 1) * 128, :].astype(F32), 0.0)
            tile = (tile * keep).astype(BF16)
            legm[t * 128 : (t + 1) * 128, :] = tile
            spec = jnp.dot(tile, xr[...], preferred_element_type=F32).astype(BF16)
            for h in range(2):
                part = spec[:, h * 512 : (h + 1) * 512]
                total = part.astype(F32) + jnp.dot(
                    part, mixer[...], preferred_element_type=F32
                )
                total = total * factor[t * 128 : (t + 1) * 128, :] * weight
                mixed[t * 128 : (t + 1) * 128, h * 512 : (h + 1) * 512] = total.astype(BF16)
        for s in range(ROUNDS):
            out = lax.dot_general(
                legm[r * 128 :, s * 128 : (s + 1) * 128],
                mixed[r * 128 :, :],
                TN,
                preferred_element_type=F32,
            )
            for p in range(LEV):
                for h in range(2):
                    half32[pl.ds(h, 128, 2), :] = out[
                        :, h * 512 + p * 128 : h * 512 + (p + 1) * 128
                    ]
                bsend.at[r, p].reshape(2 * DEGREES, 128)[s * 256 : (s + 1) * 256, :] = half32[
                    ...
                ].astype(BF16)

    table(0)
    forward(0)
    pl.semaphore_wait(barrier, PEERS - 1)
    send_forward(0)
    for d in range(1, LEV):
        vertical_copy(d).start()
    vdx[j] = vd_ref[...]
    for r in range(1, ROUNDS):
        table(r)
        forward(r)
        send_forward(r)
    build_mixer()
    for r in range(ROUNDS):
        leg_copy(r).wait()
        wait_bytes(frecv, r, frecv_sem)
        spectral(r)
        send_back(r)
    for r in range(ROUNDS):
        pltpu.make_async_copy(tab.at[r], tab_out.at[r], tab_sem.at[r]).wait()
        wait_bytes(fsend, r, fsend_sem)
        wait_bytes(bsend, r, bsend_sem)
        pltpu.make_async_copy(
            bsend.at[r, j, pl.ds(i * ROWS, ROWS)], brecv.at[r, :, me], own_sem.at[r]
        ).wait()
        wait_bytes(brecv, r, brecv_sem)


def step(grid, legendre, vd, trig, lon, waves):
    dma = pltpu.SemaphoreType.DMA
    vmem = pl.BlockSpec(memory_space=pltpu.VMEM)
    any_spec = pl.BlockSpec(memory_space=pl.ANY)
    return pl.pallas_call(
        step_kernel,
        out_shape=(
            jax.ShapeDtypeStruct((ROUNDS, ROWS, PEERS, 2, LANES), BF16),
            jax.ShapeDtypeStruct((ROUNDS, 256, LONS), BF16),
        ),
        in_specs=[any_spec, any_spec, vmem, vmem, vmem, pl.BlockSpec(memory_space=pltpu.SMEM)],
        out_specs=(any_spec, any_spec),
        scratch_shapes=[
            pltpu.VMEM((ROWS, LANES, LONS), BF16),
            pltpu.VMEM((ROUNDS, DEGREES, DEGREES), BF16),
            pltpu.VMEM((ROUNDS, 256, LONS), BF16),
            pltpu.VMEM((ROUNDS, ROWS, PEERS, 2, LANES), BF16),
            pltpu.VMEM((ROUNDS, LEV, DEGREES, 2, LANES), BF16),
            pltpu.VMEM((ROUNDS, LEV, DEGREES, 2, LANES), BF16),
            pltpu.VMEM((LEV, 48, 128), BF16),
            pltpu.VMEM((128, 128), BF16),
            pltpu.VMEM((512, 512), BF16),
            pltpu.VMEM((DEGREES, 512), F32),
            pltpu.VMEM((2 * DEGREES, 128), F32),
            pltpu.VMEM((256, 128), F32),
            pltpu.VMEM((DEGREES, 1024), BF16),
            pltpu.VMEM((DEGREES, DEGREES), BF16),
            pltpu.VMEM((DEGREES, 1024), BF16),
            dma((ROWS,)), dma((ROUNDS,)), dma((ROUNDS,)), dma, dma,
            dma((ROUNDS,)), dma((ROUNDS,)), dma((ROUNDS,)), dma((ROUNDS,)), dma((ROUNDS,)),
        ],
        compiler_params=pltpu.CompilerParams(
            collective_id=0, has_side_effects=True, vmem_limit_bytes=62 * 2**20
        ),
    )(grid, legendre, vd, trig, lon, waves)


CHUNK = 4


def inverse_kernel(back_ref, tab_ref, out_ref, lhs):
    for a in range(CHUNK):
        for r in range(ROUNDS):
            block = back_ref.at[r, a].reshape(256, 128)[...]
            lhs[a * 128 : (a + 1) * 128, r * 256 : (r + 1) * 256] = block.T
    out = jnp.dot(lhs[...], tab_ref[...], preferred_element_type=F32).astype(BF16)
    out_ref[...] = out.reshape(CHUNK, 32, 4, LONS)


def inverse(back, tab):
    return pl.pallas_call(
        inverse_kernel,
        grid=(ROWS // CHUNK,),
        out_shape=jax.ShapeDtypeStruct((ROWS, 32, 4, LONS), BF16),
        in_specs=[
            pl.BlockSpec((ROUNDS, CHUNK, PEERS, 2, LANES), lambda s: (0, s, 0, 0, 0)),
            pl.BlockSpec((LONS, LONS), lambda s: (0, 0)),
        ],
        out_specs=pl.BlockSpec((CHUNK, 32, 4, LONS), lambda s: (s, 0, 0, 0)),
        scratch_shapes=[pltpu.VMEM((CHUNK * 128, LONS), BF16)],
        compiler_params=pltpu.CompilerParams(vmem_limit_bytes=40 * 2**20),
    )(back, tab)


def per_device(grid, legendre, vertical, damping, lon_counts, wave_slots):
    points = jnp.arange(256, dtype=jnp.int32)
    points = jnp.where(points < 128, points, (points - 128) * 128 % LONS)
    waves = wave_slots.reshape(PEERS, ROUNDS).T
    phase = (waves[:, :, None] * points % LONS).astype(F32) * (2.0 * math.pi / LONS)
    scale = jnp.where(jnp.arange(256) < 128, 1.0 / math.sqrt(LONS), 1.0)
    trig = jnp.stack([jnp.cos(phase) * scale, jnp.sin(phase) * scale])
    row = lax.dynamic_update_slice_in_dim(
        jnp.zeros((128,), BF16), damping, lax.axis_index("lev") * 32, 0
    )
    vd = jnp.concatenate([vertical, jnp.broadcast_to(row, (16, 128))])
    back, tab = step(grid, legendre, vd, trig, lon_counts.reshape(1, DEGREES), wave_slots)
    return inverse(back, tab.reshape(LONS, LONS))


def solution(mesh):
    return jax.shard_map(
        per_device,
        mesh=mesh,
        in_specs=(
            P("lat", "lev", None, None),
            P("lat", None, None),
            P("lev", None),
            P("lev"),
            P(),
            P(),
        ),
        out_specs=P("lat", "lev", None, None),
        check_vma=False,
    )
```

```python
import functools
import math

import jax
import jax.numpy as jnp
from jax import lax
from jax.experimental import pallas as pl
from jax.experimental.pallas import tpu as pltpu
from jax.sharding import PartitionSpec as P

LAT, LEV = 32, 4
PEERS = LAT * LEV
ROUNDS = 5
ROWS = 20
LANES = 128
LONS = 1280
DEGREES = 640
BF16, F32 = jnp.bfloat16, jnp.float32
CHUNK = 4
PIECE = 10
MESH = pl.DeviceIdType.MESH
NT = (((1,), (1,)), ((), ()))
TN = (((0,), (0,)), ((), ()))


def step_kernel(
    grid_ref, leg_ref, vert_ref, damp_ref, lon_ref, wave_ref,
    last, part_out, tab_out,
    gv, legv, tab, fsend, frecv, bsend, brecv, vertx, dampx, damp16, vfull, mixer, factor,
    wave32, trig, pair32, half32, xr, legm, mixed, lhs, part,
    grid_sem, leg_sem, tab_sem, vsend_sem, vrecv_sem,
    fsend_sem, frecv_sem, bsend_sem, brecv_sem, own_sem, part_sem,
):
    i = lax.axis_index("lat")
    j = lax.axis_index("lev")
    me = i * LEV + j
    z, x, c = i // 8, (i // 2) % 4, i % 2

    far_z = [(z + d) % 4 * 8 for d in range(4)]
    far_x = [(x + d) % 4 * 2 for d in range(4)]
    far_c = [c, (c + 1) % 2]
    far_y = [(j + d) % LEV for d in range(LEV)]

    def to_partners(act):
        for u in range(1, 8):
            q = 45 * u % PEERS
            act(far_z[q // 32] + far_x[q // 8 % 4] + far_c[q // 4 % 2], far_y[q % 4])

        def plane(t, carry):
            for u in range(8):
                q = 45 * u % 8
                high = 13 * t + 45 * u // 8
                base = lax.rem(z + lax.div(high, 4), 4) * 8 + lax.rem(x + high, 4) * 2
                act(base + far_c[q // 4], far_y[q % 4])
            return carry

        lax.fori_loop(1, 16, plane, 0)

    def grid_copy(a):
        return pltpu.make_async_copy(
            grid_ref.at[pl.ds(a * CHUNK, CHUNK)].reshape(CHUNK * LANES, LONS),
            gv.at[a],
            grid_sem.at[a],
        )

    def leg_copy(r):
        return pltpu.make_async_copy(leg_ref.at[j * ROUNDS + r], legv.at[r], leg_sem.at[r])

    def tab_copy():
        return pltpu.make_async_copy(tab.at[ROUNDS - 1], tab_out, tab_sem)

    def landing(r):
        return brecv.at[r] if r < ROUNDS - 1 else last

    for a in range(ROWS // CHUNK):
        grid_copy(a).start()
    barrier = pltpu.get_barrier_semaphore()
    for k in range(1, PEERS):
        q = (k * 45) % PEERS
        pl.semaphore_signal(
            barrier,
            inc=1,
            device_id=(far_z[q // 32] + far_x[q // 8 % 4] + far_c[q // 4 % 2], far_y[q % 4]),
            device_id_type=MESH,
        )
    for r in range(ROUNDS):
        leg_copy(r).start()
    damp16[...] = jnp.zeros_like(damp16)
    damp16[:, 0:32] = jnp.broadcast_to(damp_ref[...].astype(F32).reshape(1, 32), (16, 32)).astype(
        BF16
    )

    def table(r):
        def spread(g, carry):
            wave32[pl.ds(g, 1), :] = jnp.full((1, 128), wave_ref[g * ROUNDS + r], jnp.int32)
            return carry

        lax.fori_loop(0, PEERS, spread, 0, unroll=8)
        wave = wave32[...].astype(F32)
        lane = lax.broadcasted_iota(jnp.int32, (PEERS, 128), 1).astype(F32)
        scale = 1.0 / math.sqrt(LONS)
        cb, sb = unit_circle(wave * lane)
        cb, sb = cb * scale, sb * scale
        trig[0], trig[1] = unit_circle(wave * lane * 128.0)
        for q in range(LONS // 128):
            ca = trig[0, :, q : q + 1]
            sa = trig[1, :, q : q + 1]
            half32[pl.ds(0, 128, 2), :] = ca * cb - sa * sb
            half32[pl.ds(1, 128, 2), :] = -(sa * cb + ca * sb)
            tab[r, :, q * 128 : (q + 1) * 128] = half32[...].astype(BF16)
        if r == ROUNDS - 1:
            tab_copy().start()

    def forward(r, first, count):
        def pair(p, carry):
            if r == 0:

                @pl.when(p % 2 == 0)
                def _():
                    grid_copy(p // 2).wait()

            rows = gv.reshape(ROWS * LANES, LONS)[pl.ds(pl.multiple_of(p * 256, 256), 256), :]
            out = lax.dot_general(tab[r], rows, NT, preferred_element_type=F32).astype(BF16)
            fsend.at[r, 2 * p].reshape(256, 128)[...] = out[:, 0:128]
            fsend.at[r, 2 * p + 1].reshape(256, 128)[...] = out[:, 128:256]
            return carry

        lax.fori_loop(first // 2, (first + count) // 2, pair, 0)

    def send_forward(r, first, count):
        def send(i2, j2):
            pltpu.make_async_remote_copy(
                src_ref=fsend.at[r, pl.ds(first, count), i2 * LEV + j2],
                dst_ref=frecv.at[r, j, pl.ds(i * ROWS + first, count)],
                send_sem=fsend_sem.at[r],
                recv_sem=frecv_sem.at[r],
                device_id=(i2, j2),
                device_id_type=MESH,
            ).start()

        to_partners(send)
        frecv[r, j, pl.ds(i * ROWS + first, count)] = fsend[r, first : first + count, me]

    def send_back(r):
        def send(i2, j2):
            pltpu.make_async_remote_copy(
                src_ref=bsend.at[r, j2, pl.ds(i2 * ROWS, ROWS)],
                dst_ref=landing(r).at[:, me],
                send_sem=bsend_sem.at[r],
                recv_sem=brecv_sem.at[r],
                device_id=(i2, j2),
                device_id_type=MESH,
            ).start()

        to_partners(send)
        if r < ROUNDS - 1:
            brecv[r, :, me] = bsend[r, j, pl.ds(i * ROWS, ROWS)]
        else:
            own_copy().start()

    def own_copy():
        return pltpu.make_async_copy(
            bsend.at[ROUNDS - 1, j, pl.ds(i * ROWS, ROWS)], last.at[:, me], own_sem
        )

    def part_copy(s):
        return pltpu.make_async_copy(
            part.at[s % 2], part_out.at[pl.ds(s * CHUNK * 128, CHUNK * 128)], part_sem.at[s % 2]
        )

    def wait_bytes(ref, r, sem):
        most = ref.reshape(ROWS * PEERS, 2, LANES).at[pl.ds(0, ROWS * (PEERS - 1))]
        pltpu.make_async_copy(most, most, sem.at[r]).wait()

    def level_copy(src, dst, s, d):
        return pltpu.make_async_remote_copy(
            src_ref=src,
            dst_ref=dst.at[j],
            send_sem=vsend_sem.at[s],
            recv_sem=vrecv_sem.at[s],
            device_id=(i, (j + d) % LEV),
            device_id_type=MESH,
        )

    def build_mixer():
        for s, ref in enumerate((vertx, dampx)):
            three = ref.at[pl.ds(0, LEV - 1)]
            pltpu.make_async_copy(three, three, vrecv_sem.at[s]).wait()
            pltpu.make_async_copy(three, three, vsend_sem.at[s]).wait()
        for p in range(LEV):
            vfull[p * 32 : (p + 1) * 32, :] = vertx[p]
        row = lax.broadcasted_iota(jnp.int32, (512, 128), 0)
        col = lax.broadcasted_iota(jnp.int32, (512, 128), 1)
        pick = jnp.where(row // 4 == col, 1.0, 0.0).astype(BF16)
        tall = lax.dot_general(pick, vfull[...], NT, preferred_element_type=F32).astype(BF16)
        wide = lax.dot_general(tall, pick, NT, preferred_element_type=F32)
        row = lax.broadcasted_iota(jnp.int32, (512, 512), 0)
        col = lax.broadcasted_iota(jnp.int32, (512, 512), 1)
        mixer[...] = jnp.where(row % 4 == col % 4, wide, 0.0).astype(BF16)
        near = jnp.where(row[:, 0:128] // 4 % 32 == col[:, 0:128], 1.0, 0.0).astype(BF16)
        lane = lax.broadcasted_iota(jnp.int32, (16, 512), 1)
        damp = jnp.zeros((16, 512), F32)
        for p in range(LEV):
            found = lax.dot_general(dampx[p], near, NT, preferred_element_type=F32)
            damp = damp + jnp.where(lane // 128 == p, found, 0.0)
        damp = damp[0:1, :]
        for t in range(ROUNDS):
            n = (lax.broadcasted_iota(jnp.int32, (128, 512), 0) + 128 * t).astype(F32)
            ratio = n * (n + 1.0) / float(DEGREES * (DEGREES - 1))
            factor[t * 128 : (t + 1) * 128, :] = 1.0 / (1.0 + damp * (ratio * ratio))

    def spectral(r):
        wave = wave_ref[me * ROUNDS + r]
        weight = jnp.where(wave == 0, 1.0, 2.0).astype(F32)
        for p in range(LEV):
            pair32[...] = frecv.at[r, p].reshape(2 * DEGREES, 128)[...].astype(F32)
            for h in range(2):
                xr[:, h * 512 + p * 128 : h * 512 + (p + 1) * 128] = pair32[
                    pl.ds(h, DEGREES, 2), :
                ].astype(BF16)
        keep = jnp.where(2 * wave < lon_ref[...], 1.0, 0.0).reshape(1, DEGREES)
        for t in range(r, ROUNDS):
            n = lax.broadcasted_iota(jnp.int32, (128, DEGREES), 0) + 128 * t
            tile = jnp.where(n >= wave, legv[r, t * 128 : (t + 1) * 128, :].astype(F32), 0.0)
            tile = (tile * keep).astype(BF16)
            legm[t * 128 : (t + 1) * 128, :] = tile
            spec = jnp.dot(tile, xr[...], preferred_element_type=F32).astype(BF16)
            for h in range(2):
                part = spec[:, h * 512 : (h + 1) * 512]
                total = part.astype(F32) + jnp.dot(
                    part, mixer[...], preferred_element_type=F32
                )
                total = total * factor[t * 128 : (t + 1) * 128, :] * weight
                mixed[t * 128 : (t + 1) * 128, h * 512 : (h + 1) * 512] = total.astype(BF16)
        for s in range(ROUNDS):
            out = lax.dot_general(
                legm[r * 128 :, s * 128 : (s + 1) * 128],
                mixed[r * 128 :, :],
                TN,
                preferred_element_type=F32,
            )
            for p in range(LEV):
                for h in range(2):
                    half32[pl.ds(h, 128, 2), :] = out[
                        :, h * 512 + p * 128 : h * 512 + (p + 1) * 128
                    ]
                bsend.at[r, p].reshape(2 * DEGREES, 128)[s * 256 : (s + 1) * 256, :] = half32[
                    ...
                ].astype(BF16)

    table(0)
    forward(0, 0, 12)
    pl.semaphore_wait(barrier, PEERS - 1)
    send_forward(0, 0, 12)
    forward(0, 12, 8)
    send_forward(0, 12, 8)
    for d in range(1, LEV):
        level_copy(vert_ref, vertx, 0, d).start()
        level_copy(damp16, dampx, 1, d).start()
    vertx[j] = vert_ref[...]
    dampx[j] = damp16[...]
    for r in range(1, ROUNDS):
        table(r)
        forward(r, 0, ROWS)
        send_forward(r, 0, ROWS)
    build_mixer()
    for r in range(ROUNDS):
        leg_copy(r).wait()
        wait_bytes(frecv.at[r], r, frecv_sem)
        spectral(r)
        send_back(r)
    for r in range(ROUNDS - 1):
        wait_bytes(brecv.at[r], r, brecv_sem)
    for s in range(ROWS // CHUNK):
        for a in range(CHUNK):
            for r in range(ROUNDS - 1):
                block = brecv.at[r, s * CHUNK + a].reshape(256, 128)[...]
                lhs[a * 128 : (a + 1) * 128, r * 256 : (r + 1) * 256] = block.T
        if s >= 2:
            part_copy(s - 2).wait()
        part[s % 2] = jnp.dot(
            lhs[...],
            tab[0 : ROUNDS - 1].reshape((ROUNDS - 1) * 256, LONS),
            preferred_element_type=F32,
        ).astype(BF16)
        part_copy(s).start()
    for s in range(ROWS // CHUNK - 2, ROWS // CHUNK):
        part_copy(s).wait()
    tab_copy().wait()
    for r in range(ROUNDS):
        wait_bytes(fsend.at[r], r, fsend_sem)
        wait_bytes(bsend.at[r], r, bsend_sem)
    own_copy().wait()
    wait_bytes(last, ROUNDS - 1, brecv_sem)


def unit_circle(steps):
    turns = jnp.floor(steps * (1.0 / LONS))
    rest = steps - turns * LONS
    rest = jnp.where(rest < 0.0, rest + LONS, rest)
    rest = jnp.where(rest >= LONS, rest - LONS, rest)
    quarter = jnp.floor(rest * (4.0 / LONS) + 0.5)
    y = (rest - quarter * (LONS // 4)) * (2.0 * math.pi / LONS)
    y2 = y * y
    sine = y * (1 + y2 * (-1 / 6 + y2 * (1 / 120 + y2 * (-1 / 5040 + y2 * (1 / 362880)))))
    cosine = 1 + y2 * (
        -1 / 2 + y2 * (1 / 24 + y2 * (-1 / 720 + y2 * (1 / 40320 - y2 * (1 / 3628800))))
    )
    odd = (quarter == 1.0) | (quarter == 3.0)
    first = jnp.where(odd, sine, cosine)
    second = jnp.where(odd, cosine, sine)
    back = (quarter == 2.0) | (quarter == 3.0)
    left = (quarter == 1.0) | (quarter == 2.0)
    return jnp.where(left, -first, first), jnp.where(back, -second, second)


def step(grid, legendre, vertical, damp, lon, waves):
    dma = pltpu.SemaphoreType.DMA
    vmem = pl.BlockSpec(memory_space=pltpu.VMEM)
    any_spec = pl.BlockSpec(memory_space=pl.ANY)
    return pl.pallas_call(
        step_kernel,
        out_shape=(
            jax.ShapeDtypeStruct((ROWS, PEERS, 2, LANES), BF16),
            jax.ShapeDtypeStruct((ROWS * LANES, LONS), BF16),
            jax.ShapeDtypeStruct((256, LONS), BF16),
        ),
        in_specs=[any_spec, any_spec, vmem, vmem, vmem, pl.BlockSpec(memory_space=pltpu.SMEM)],
        out_specs=(any_spec, any_spec, any_spec),
        scratch_shapes=[
            pltpu.VMEM((ROWS // CHUNK, CHUNK * LANES, LONS), BF16),
            pltpu.VMEM((ROUNDS, DEGREES, DEGREES), BF16),
            pltpu.VMEM((ROUNDS, 256, LONS), BF16),
            pltpu.VMEM((ROUNDS, ROWS, PEERS, 2, LANES), BF16),
            pltpu.VMEM((ROUNDS, LEV, DEGREES, 2, LANES), BF16),
            pltpu.VMEM((ROUNDS, LEV, DEGREES, 2, LANES), BF16),
            pltpu.VMEM((ROUNDS - 1, ROWS, PEERS, 2, LANES), BF16),
            pltpu.VMEM((LEV, 32, 128), BF16),
            pltpu.VMEM((LEV, 16, 128), BF16),
            pltpu.VMEM((16, 128), BF16),
            pltpu.VMEM((128, 128), BF16),
            pltpu.VMEM((512, 512), BF16),
            pltpu.VMEM((DEGREES, 512), F32),
            pltpu.VMEM((PEERS, 128), jnp.int32),
            pltpu.VMEM((2, PEERS, 128), F32),
            pltpu.VMEM((2 * DEGREES, 128), F32),
            pltpu.VMEM((256, 128), F32),
            pltpu.VMEM((DEGREES, 1024), BF16),
            pltpu.VMEM((DEGREES, DEGREES), BF16),
            pltpu.VMEM((DEGREES, 1024), BF16),
            pltpu.VMEM((CHUNK * 128, (ROUNDS - 1) * 256), BF16),
            pltpu.VMEM((2, CHUNK * 128, LONS), BF16),
            dma((ROWS // CHUNK,)), dma((ROUNDS,)), dma, dma((2,)), dma((2,)),
            dma((ROUNDS,)), dma((ROUNDS,)), dma((ROUNDS,)), dma((ROUNDS,)), dma, dma((2,)),
        ],
        compiler_params=pltpu.CompilerParams(
            collective_id=0, has_side_effects=True, vmem_limit_bytes=62 * 2**20
        ),
    )(grid, legendre, vertical, damp, lon, waves)


def finish_kernel(last_ref, tab_ref, part_ref, out_ref, lhs, stage, sem):
    s = pl.program_id(0)
    slot = s % 2

    def out_copy(step, where):
        return pltpu.make_async_copy(
            stage.at[where],
            out_ref.at[pl.ds(step * PIECE, PIECE)].reshape(PIECE * LANES, LONS),
            sem.at[where],
        )

    for a in range(PIECE):
        lhs[a * 128 : (a + 1) * 128, :] = last_ref.at[a].reshape(256, 128)[...].T

    @pl.when(s >= 2)
    def _():
        out_copy(s - 2, slot).wait()

    out = jnp.dot(lhs[...], tab_ref[...], preferred_element_type=F32)
    stage[slot] = (out + part_ref[...].astype(F32)).astype(BF16)
    out_copy(s, slot).start()

    @pl.when(s == pl.num_programs(0) - 1)
    def _():
        out_copy(s - 1, 1 - slot).wait()
        out_copy(s, slot).wait()


def finish(last, part, tab):
    return pl.pallas_call(
        finish_kernel,
        grid=(ROWS // PIECE,),
        out_shape=jax.ShapeDtypeStruct((ROWS, 32, 4, LONS), BF16),
        in_specs=[
            pl.BlockSpec((PIECE, PEERS, 2, LANES), lambda s: (s, 0, 0, 0)),
            pl.BlockSpec((256, LONS), lambda s: (0, 0)),
            pl.BlockSpec((PIECE * 128, LONS), lambda s: (s, 0)),
        ],
        out_specs=pl.BlockSpec(memory_space=pl.ANY),
        scratch_shapes=[
            pltpu.VMEM((PIECE * 128, 256), BF16),
            pltpu.VMEM((2, PIECE * 128, LONS), BF16),
            pltpu.SemaphoreType.DMA((2,)),
        ],
        compiler_params=pltpu.CompilerParams(vmem_limit_bytes=62 * 2**20),
    )(last, tab, part)


def per_device(grid, legendre, vertical, damping, lon_counts, wave_slots):
    last, part, tab = step(grid, legendre, vertical, damping, lon_counts, wave_slots)
    return finish(last, part, tab)


def solution(mesh):
    return jax.shard_map(
        per_device,
        mesh=mesh,
        in_specs=(
            P("lat", "lev", None, None),
            P("lat", None, None),
            P("lev", None),
            P("lev"),
            P(),
            P(),
        ),
        out_specs=P("lat", "lev", None, None),
        check_vma=False,
    )
```

```python
import functools
import math

import jax
import jax.numpy as jnp
from jax import lax
from jax.experimental import pallas as pl
from jax.experimental.pallas import tpu as pltpu
from jax.sharding import PartitionSpec as P

LAT, LEV = 32, 4
PEERS = LAT * LEV
ROUNDS = 5
ROWS = 20
LANES = 128
LONS = 1280
DEGREES = 640
BF16, F32 = jnp.bfloat16, jnp.float32
CHUNK = 4
PIECE = 10
MESH = pl.DeviceIdType.MESH
NT = (((1,), (1,)), ((), ()))
TN = (((0,), (0,)), ((), ()))


def step_kernel(
    grid_ref, leg_ref, vert_ref, damp_hbm, lon_hbm, wave_hbm,
    last, part_out, tab_out,
    gv, legv, tab, sent, frecv, brecv, vertx, dampx, damp16, vfull, mixer, factor,
    wave_ref, lon_ref, damp_ref, wave32, trig, pair32, half32, xr, legm, mixed, lhs, part,
    grid_sem, leg_sem, tab_sem, vsend_sem, vrecv_sem,
    fsend_sem, frecv_sem, bsend_sem, brecv_sem, own_sem, part_sem, small_sem,
):
    i = lax.axis_index("lat")
    j = lax.axis_index("lev")
    me = i * LEV + j
    z, x, c = i // 8, (i // 2) % 4, i % 2

    far_z = [(z + d) % 4 * 8 for d in range(4)]
    far_x = [(x + d) % 4 * 2 for d in range(4)]
    far_c = [c, (c + 1) % 2]
    far_y = [(j + d) % LEV for d in range(LEV)]

    def to_partners(act):
        for u in range(1, 8):
            q = 45 * u % PEERS
            act(far_z[q // 32] + far_x[q // 8 % 4] + far_c[q // 4 % 2], far_y[q % 4])

        def plane(t, carry):
            for u in range(8):
                q = 45 * u % 8
                high = 13 * t + 45 * u // 8
                base = lax.rem(z + lax.div(high, 4), 4) * 8 + lax.rem(x + high, 4) * 2
                act(base + far_c[q // 4], far_y[q % 4])
            return carry

        lax.fori_loop(1, 16, plane, 0)

    def grid_copy(a):
        return pltpu.make_async_copy(
            grid_ref.at[pl.ds(a * CHUNK, CHUNK)].reshape(CHUNK * LANES, LONS),
            gv.at[a],
            grid_sem.at[a],
        )

    def leg_copy(r):
        return pltpu.make_async_copy(leg_ref.at[j * ROUNDS + r], legv.at[r], leg_sem.at[r])

    def tab_copy():
        return pltpu.make_async_copy(tab.at[ROUNDS - 1], tab_out, tab_sem)

    def landing(r):
        return brecv.at[r] if r < ROUNDS - 1 else last

    small = [
        pltpu.make_async_copy(wave_hbm, wave_ref, small_sem.at[0]),
        pltpu.make_async_copy(lon_hbm, lon_ref, small_sem.at[1]),
        pltpu.make_async_copy(damp_hbm, damp_ref, small_sem.at[2]),
        pltpu.make_async_copy(vert_ref, vertx.at[j], small_sem.at[3]),
    ]
    small[0].start()
    for a in range(ROWS // CHUNK):
        grid_copy(a).start()
    barrier = pltpu.get_barrier_semaphore()
    for k in range(1, PEERS):
        q = (k * 45) % PEERS
        pl.semaphore_signal(
            barrier,
            inc=1,
            device_id=(far_z[q // 32] + far_x[q // 8 % 4] + far_c[q // 4 % 2], far_y[q % 4]),
            device_id_type=MESH,
        )
    def table(r):
        def spread(g, carry):
            wave32[pl.ds(g, 1), :] = jnp.full((1, 128), wave_ref[g * ROUNDS + r], jnp.int32)
            return carry

        lax.fori_loop(0, PEERS, spread, 0, unroll=8)
        wave = wave32[...].astype(F32)
        lane = lax.broadcasted_iota(jnp.int32, (PEERS, 128), 1).astype(F32)
        scale = 1.0 / math.sqrt(LONS)
        cb, sb = unit_circle(wave * lane)
        cb, sb = cb * scale, sb * scale
        trig[0], trig[1] = unit_circle(wave * lane * 128.0)
        for q in range(LONS // 128):
            ca = trig[0, :, q : q + 1]
            sa = trig[1, :, q : q + 1]
            half32[pl.ds(0, 128, 2), :] = ca * cb - sa * sb
            half32[pl.ds(1, 128, 2), :] = -(sa * cb + ca * sb)
            tab[r, :, q * 128 : (q + 1) * 128] = half32[...].astype(BF16)
        if r == ROUNDS - 1:
            tab_copy().start()

    def by_row(r):
        return sent.at[r].reshape(ROWS, PEERS, 2, LANES)

    def by_level(r):
        return sent.at[r].reshape(LEV, DEGREES, 2, LANES)

    def forward(r, first, count):
        def pair(p, carry):
            if r == 0:

                @pl.when(p % 2 == 0)
                def _():
                    grid_copy(p // 2).wait()

            rows = gv.reshape(ROWS * LANES, LONS)[pl.ds(pl.multiple_of(p * 256, 256), 256), :]
            out = lax.dot_general(tab[r], rows, NT, preferred_element_type=F32).astype(BF16)
            for h in range(2):
                place = sent.at[r, pl.ds((2 * p + h) * PEERS, PEERS)]
                place.reshape(256, 128)[...] = out[:, h * 128 : (h + 1) * 128]
            return carry

        lax.fori_loop(first // 2, (first + count) // 2, pair, 0)

    def send_forward(r, first, count):
        def send(i2, j2):
            pltpu.make_async_remote_copy(
                src_ref=by_row(r).at[pl.ds(first, count), i2 * LEV + j2],
                dst_ref=frecv.at[r, j, pl.ds(i * ROWS + first, count)],
                send_sem=fsend_sem.at[r],
                recv_sem=frecv_sem.at[r],
                device_id=(i2, j2),
                device_id_type=MESH,
            ).start()

        to_partners(send)
        frecv[r, j, pl.ds(i * ROWS + first, count)] = by_row(r)[first : first + count, me]

    def send_back(r):
        def send(i2, j2):
            pltpu.make_async_remote_copy(
                src_ref=by_level(r).at[j2, pl.ds(i2 * ROWS, ROWS)],
                dst_ref=landing(r).at[:, me],
                send_sem=bsend_sem.at[r],
                recv_sem=brecv_sem.at[r],
                device_id=(i2, j2),
                device_id_type=MESH,
            ).start()

        to_partners(send)
        if r < ROUNDS - 1:
            brecv[r, :, me] = by_level(r)[j, pl.ds(i * ROWS, ROWS)]
        else:
            own_copy().start()

    def own_copy():
        return pltpu.make_async_copy(
            by_level(ROUNDS - 1).at[j, pl.ds(i * ROWS, ROWS)], last.at[:, me], own_sem
        )

    def part_copy(s):
        return pltpu.make_async_copy(
            part.at[s % 2], part_out.at[pl.ds(s * CHUNK * 128, CHUNK * 128)], part_sem.at[s % 2]
        )

    def wait_bytes(ref, r, sem):
        most = ref.reshape(ROWS * PEERS, 2, LANES).at[pl.ds(0, ROWS * (PEERS - 1))]
        pltpu.make_async_copy(most, most, sem.at[r]).wait()

    def level_copy(src, dst, s, d):
        return pltpu.make_async_remote_copy(
            src_ref=src,
            dst_ref=dst.at[j],
            send_sem=vsend_sem.at[s],
            recv_sem=vrecv_sem.at[s],
            device_id=(i, (j + d) % LEV),
            device_id_type=MESH,
        )

    def build_mixer():
        for s, ref in enumerate((vertx, dampx)):
            three = ref.at[pl.ds(0, LEV - 1)]
            pltpu.make_async_copy(three, three, vrecv_sem.at[s]).wait()
            pltpu.make_async_copy(three, three, vsend_sem.at[s]).wait()
        for p in range(LEV):
            vfull[p * 32 : (p + 1) * 32, :] = vertx[p]
        row = lax.broadcasted_iota(jnp.int32, (512, 128), 0)
        col = lax.broadcasted_iota(jnp.int32, (512, 128), 1)
        pick = jnp.where(row // 4 == col, 1.0, 0.0).astype(BF16)
        tall = lax.dot_general(pick, vfull[...], NT, preferred_element_type=F32).astype(BF16)
        wide = lax.dot_general(tall, pick, NT, preferred_element_type=F32)
        row = lax.broadcasted_iota(jnp.int32, (512, 512), 0)
        col = lax.broadcasted_iota(jnp.int32, (512, 512), 1)
        mixer[...] = jnp.where(row % 4 == col % 4, wide, 0.0).astype(BF16)
        near = jnp.where(row[:, 0:128] // 4 % 32 == col[:, 0:128], 1.0, 0.0).astype(BF16)
        lane = lax.broadcasted_iota(jnp.int32, (16, 512), 1)
        damp = jnp.zeros((16, 512), F32)
        for p in range(LEV):
            found = lax.dot_general(dampx[p], near, NT, preferred_element_type=F32)
            damp = damp + jnp.where(lane // 128 == p, found, 0.0)
        damp = damp[0:1, :]
        for t in range(ROUNDS):
            n = (lax.broadcasted_iota(jnp.int32, (128, 512), 0) + 128 * t).astype(F32)
            ratio = n * (n + 1.0) / float(DEGREES * (DEGREES - 1))
            factor[t * 128 : (t + 1) * 128, :] = 1.0 / (1.0 + damp * (ratio * ratio))

    def spectral(r):
        wave = wave_ref[me * ROUNDS + r]
        weight = jnp.where(wave == 0, 1.0, 2.0).astype(F32)
        for p in range(LEV):
            pair32[...] = frecv.at[r, p].reshape(2 * DEGREES, 128)[...].astype(F32)
            for h in range(2):
                xr[:, h * 512 + p * 128 : h * 512 + (p + 1) * 128] = pair32[
                    pl.ds(h, DEGREES, 2), :
                ].astype(BF16)
        keep = jnp.where(2 * wave < lon_ref[...], 1.0, 0.0).reshape(1, DEGREES)
        for t in range(r, ROUNDS):
            n = lax.broadcasted_iota(jnp.int32, (128, DEGREES), 0) + 128 * t
            tile = jnp.where(n >= wave, legv[r, t * 128 : (t + 1) * 128, :].astype(F32), 0.0)
            tile = (tile * keep).astype(BF16)
            legm[t * 128 : (t + 1) * 128, :] = tile
            spec = jnp.dot(tile, xr[...], preferred_element_type=F32).astype(BF16)
            for h in range(2):
                part = spec[:, h * 512 : (h + 1) * 512]
                total = part.astype(F32) + jnp.dot(
                    part, mixer[...], preferred_element_type=F32
                )
                total = total * factor[t * 128 : (t + 1) * 128, :] * weight
                mixed[t * 128 : (t + 1) * 128, h * 512 : (h + 1) * 512] = total.astype(BF16)
        for s in range(ROUNDS):
            out = lax.dot_general(
                legm[r * 128 :, s * 128 : (s + 1) * 128],
                mixed[r * 128 :, :],
                TN,
                preferred_element_type=F32,
            )
            for p in range(LEV):
                for h in range(2):
                    half32[pl.ds(h, 128, 2), :] = out[
                        :, h * 512 + p * 128 : h * 512 + (p + 1) * 128
                    ]
                place = sent.at[r, pl.ds(p * DEGREES + s * 128, 128)]
                place.reshape(256, 128)[...] = half32[...].astype(BF16)

    small[0].wait()
    table(0)
    forward(0, 0, 8)
    pl.semaphore_wait(barrier, PEERS - 1)
    send_forward(0, 0, 8)
    forward(0, 8, 12)
    send_forward(0, 8, 12)
    for copy in small[1:]:
        copy.start()
    for r in range(ROUNDS):
        leg_copy(r).start()
    for copy in small[1:]:
        copy.wait()
    damp16[...] = jnp.zeros_like(damp16)
    damp16[:, 0:32] = jnp.broadcast_to(damp_ref[...].astype(F32).reshape(1, 32), (16, 32)).astype(
        BF16
    )
    for d in range(1, LEV):
        level_copy(vert_ref, vertx, 0, d).start()
        level_copy(damp16, dampx, 1, d).start()
    dampx[j] = damp16[...]
    for r in range(1, ROUNDS):
        table(r)
        forward(r, 0, ROWS)
        send_forward(r, 0, ROWS)
    build_mixer()
    for r in range(ROUNDS):
        leg_copy(r).wait()
        wait_bytes(sent.at[r], r, fsend_sem)
        wait_bytes(frecv.at[r], r, frecv_sem)
        spectral(r)
        send_back(r)
    for r in range(ROUNDS - 1):
        wait_bytes(brecv.at[r], r, brecv_sem)
    for s in range(ROWS // CHUNK):
        for a in range(CHUNK):
            for r in range(ROUNDS - 1):
                block = brecv.at[r, s * CHUNK + a].reshape(256, 128)[...]
                lhs[a * 128 : (a + 1) * 128, r * 256 : (r + 1) * 256] = block.T
        if s >= 2:
            part_copy(s - 2).wait()
        part[s % 2] = jnp.dot(
            lhs[...],
            tab[0 : ROUNDS - 1].reshape((ROUNDS - 1) * 256, LONS),
            preferred_element_type=F32,
        ).astype(BF16)
        part_copy(s).start()
    for s in range(ROWS // CHUNK - 2, ROWS // CHUNK):
        part_copy(s).wait()
    tab_copy().wait()
    for r in range(ROUNDS):
        wait_bytes(sent.at[r], r, bsend_sem)
    own_copy().wait()
    wait_bytes(last, ROUNDS - 1, brecv_sem)


def unit_circle(steps):
    turns = jnp.floor(steps * (1.0 / LONS))
    rest = steps - turns * LONS
    rest = jnp.where(rest < 0.0, rest + LONS, rest)
    rest = jnp.where(rest >= LONS, rest - LONS, rest)
    quarter = jnp.floor(rest * (4.0 / LONS) + 0.5)
    y = (rest - quarter * (LONS // 4)) * (2.0 * math.pi / LONS)
    y2 = y * y
    sine = y * (1 + y2 * (-1 / 6 + y2 * (1 / 120 + y2 * (-1 / 5040 + y2 * (1 / 362880)))))
    cosine = 1 + y2 * (
        -1 / 2 + y2 * (1 / 24 + y2 * (-1 / 720 + y2 * (1 / 40320 - y2 * (1 / 3628800))))
    )
    odd = (quarter == 1.0) | (quarter == 3.0)
    first = jnp.where(odd, sine, cosine)
    second = jnp.where(odd, cosine, sine)
    back = (quarter == 2.0) | (quarter == 3.0)
    left = (quarter == 1.0) | (quarter == 2.0)
    return jnp.where(left, -first, first), jnp.where(back, -second, second)


def step(grid, legendre, vertical, damp, lon, waves):
    dma = pltpu.SemaphoreType.DMA
    any_spec = pl.BlockSpec(memory_space=pl.ANY)
    return pl.pallas_call(
        step_kernel,
        out_shape=(
            jax.ShapeDtypeStruct((ROWS, PEERS, 2, LANES), BF16),
            jax.ShapeDtypeStruct((ROWS * LANES, LONS), BF16),
            jax.ShapeDtypeStruct((256, LONS), BF16),
        ),
        in_specs=[pl.BlockSpec(memory_space=pltpu.HBM)] * 6,
        out_specs=(any_spec, any_spec, any_spec),
        scratch_shapes=[
            pltpu.VMEM((ROWS // CHUNK, CHUNK * LANES, LONS), BF16),
            pltpu.VMEM((ROUNDS, DEGREES, DEGREES), BF16),
            pltpu.VMEM((ROUNDS, 256, LONS), BF16),
            pltpu.VMEM((ROUNDS, ROWS * PEERS, 2, LANES), BF16),
            pltpu.VMEM((ROUNDS, LEV, DEGREES, 2, LANES), BF16),
            pltpu.VMEM((ROUNDS - 1, ROWS, PEERS, 2, LANES), BF16),
            pltpu.VMEM((LEV, 32, 128), BF16),
            pltpu.VMEM((LEV, 16, 128), BF16),
            pltpu.VMEM((16, 128), BF16),
            pltpu.VMEM((128, 128), BF16),
            pltpu.VMEM((512, 512), BF16),
            pltpu.VMEM((DEGREES, 512), F32),
            pltpu.SMEM((DEGREES,), jnp.int32),
            pltpu.VMEM((DEGREES,), jnp.int32),
            pltpu.VMEM((32,), BF16),
            pltpu.VMEM((PEERS, 128), jnp.int32),
            pltpu.VMEM((2, PEERS, 128), F32),
            pltpu.VMEM((2 * DEGREES, 128), F32),
            pltpu.VMEM((256, 128), F32),
            pltpu.VMEM((DEGREES, 1024), BF16),
            pltpu.VMEM((DEGREES, DEGREES), BF16),
            pltpu.VMEM((DEGREES, 1024), BF16),
            pltpu.VMEM((CHUNK * 128, (ROUNDS - 1) * 256), BF16),
            pltpu.VMEM((2, CHUNK * 128, LONS), BF16),
            dma((ROWS // CHUNK,)), dma((ROUNDS,)), dma, dma((2,)), dma((2,)),
            dma((ROUNDS,)), dma((ROUNDS,)), dma((ROUNDS,)), dma((ROUNDS,)), dma, dma((2,)), dma((4,)),
        ],
        compiler_params=pltpu.CompilerParams(
            collective_id=0, has_side_effects=True, vmem_limit_bytes=67043328
        ),
    )(grid, legendre, vertical, damp, lon, waves)


def finish_kernel(last_ref, tab_ref, part_ref, out_ref, stage, sem):
    s = pl.program_id(0)
    slot = s % 2

    def out_copy(step, where):
        return pltpu.make_async_copy(
            stage.at[where],
            out_ref.at[pl.ds(step * PIECE, PIECE)].reshape(PIECE * LANES, LONS),
            sem.at[where],
        )

    @pl.when(s >= 2)
    def _():
        out_copy(s - 2, slot).wait()

    for a in range(PIECE):
        block = last_ref.at[a].reshape(256, 128)[...]
        out = lax.dot_general(block, tab_ref[...], TN, preferred_element_type=F32)
        rows = slice(a * 128, (a + 1) * 128)
        stage[slot, rows, :] = (out + part_ref[rows, :].astype(F32)).astype(BF16)
    out_copy(s, slot).start()

    @pl.when(s == pl.num_programs(0) - 1)
    def _():
        out_copy(s - 1, 1 - slot).wait()
        out_copy(s, slot).wait()


def finish(last, part, tab):
    return pl.pallas_call(
        finish_kernel,
        grid=(ROWS // PIECE,),
        out_shape=jax.ShapeDtypeStruct((ROWS, 32, 4, LONS), BF16),
        in_specs=[
            pl.BlockSpec((PIECE, PEERS, 2, LANES), lambda s: (s, 0, 0, 0)),
            pl.BlockSpec((256, LONS), lambda s: (0, 0)),
            pl.BlockSpec((PIECE * 128, LONS), lambda s: (s, 0)),
        ],
        out_specs=pl.BlockSpec(memory_space=pl.ANY),
        scratch_shapes=[
            pltpu.VMEM((2, PIECE * 128, LONS), BF16),
            pltpu.SemaphoreType.DMA((2,)),
        ],
        compiler_params=pltpu.CompilerParams(vmem_limit_bytes=62 * 2**20),
    )(last, tab, part)


def per_device(grid, legendre, vertical, damping, lon_counts, wave_slots):
    last, part, tab = step(grid, legendre, vertical, damping, lon_counts, wave_slots)
    return finish(last, part, tab)


def solution(mesh):
    return jax.shard_map(
        per_device,
        mesh=mesh,
        in_specs=(
            P("lat", "lev", None, None),
            P("lat", None, None),
            P("lev", None),
            P("lev"),
            P(),
            P(),
        ),
        out_specs=P("lat", "lev", None, None),
        check_vma=False,
    )
```

```python
import functools
import math

import jax
import jax.numpy as jnp
from jax import lax
from jax.experimental import pallas as pl
from jax.experimental.pallas import tpu as pltpu
from jax.sharding import PartitionSpec as P

LAT, LEV = 32, 4
PEERS = LAT * LEV
ROUNDS = 5
ROWS = 20
LANES = 128
LONS = 1280
DEGREES = 640
BF16, F32 = jnp.bfloat16, jnp.float32
CHUNK = 4
PIECE = 10
MESH = pl.DeviceIdType.MESH
NT = (((1,), (1,)), ((), ()))
TN = (((0,), (0,)), ((), ()))


def step_kernel(
    grid_ref, leg_ref, vert_ref, damp_hbm, lon_hbm, wave_hbm,
    last, part_out, tab_out,
    gv, legv, tab, sent, frecv, brecv, vertx, dampx, damp16, vfull, mixer, factor,
    wave_ref, lon_ref, damp_ref, wave32, trig, pair32, half32, xr, legm, mixed, lhs, part,
    grid_sem, leg_sem, tab_sem, vsend_sem, vrecv_sem,
    fsend_sem, frecv_sem, bsend_sem, brecv_sem, own_sem, part_sem, small_sem,
):
    i = lax.axis_index("lat")
    j = lax.axis_index("lev")
    me = i * LEV + j
    z, x, c = i // 8, (i // 2) % 4, i % 2

    far_z = [(z + d) % 4 * 8 for d in range(4)]
    far_x = [(x + d) % 4 * 2 for d in range(4)]
    far_c = [c, (c + 1) % 2]
    far_y = [(j + d) % LEV for d in range(LEV)]

    def to_partners(act):
        for u in range(1, 8):
            q = 45 * u % PEERS
            act(far_z[q // 32] + far_x[q // 8 % 4] + far_c[q // 4 % 2], far_y[q % 4])

        def plane(t, carry):
            for u in range(8):
                q = 45 * u % 8
                high = 13 * t + 45 * u // 8
                base = lax.rem(z + lax.div(high, 4), 4) * 8 + lax.rem(x + high, 4) * 2
                act(base + far_c[q // 4], far_y[q % 4])
            return carry

        lax.fori_loop(1, 16, plane, 0)

    def grid_copy(a):
        return pltpu.make_async_copy(
            grid_ref.at[pl.ds(a * CHUNK, CHUNK)].reshape(CHUNK * LANES, LONS),
            gv.at[a],
            grid_sem.at[a],
        )

    def leg_copy(r):
        return pltpu.make_async_copy(leg_ref.at[j * ROUNDS + r], legv.at[r], leg_sem.at[r])

    def tab_copy():
        return pltpu.make_async_copy(tab.at[ROUNDS - 1], tab_out, tab_sem)

    def landing(r):
        return brecv.at[r] if r < ROUNDS - 1 else last

    barrier = pltpu.get_barrier_semaphore()
    for q in sorted(range(1, PEERS), key=hops, reverse=True):
        pl.semaphore_signal(
            barrier,
            inc=1,
            device_id=(far_z[q // 32] + far_x[q // 8 % 4] + far_c[q // 4 % 2], far_y[q % 4]),
            device_id_type=MESH,
        )
    small = [
        pltpu.make_async_copy(wave_hbm, wave_ref, small_sem.at[0]),
        pltpu.make_async_copy(lon_hbm, lon_ref, small_sem.at[1]),
        pltpu.make_async_copy(damp_hbm, damp_ref, small_sem.at[2]),
        pltpu.make_async_copy(vert_ref, vertx.at[j], small_sem.at[3]),
    ]
    small[0].start()
    for a in range(ROWS // CHUNK):
        grid_copy(a).start()
    def table(r):
        def spread(g, carry):
            wave32[pl.ds(g, 1), :] = jnp.full((1, 128), wave_ref[g * ROUNDS + r], jnp.int32)
            return carry

        lax.fori_loop(0, PEERS, spread, 0, unroll=8)
        wave = wave32[...].astype(F32)
        lane = lax.broadcasted_iota(jnp.int32, (PEERS, 128), 1).astype(F32)
        scale = 1.0 / math.sqrt(LONS)
        cb, sb = unit_circle(wave * lane)
        cb, sb = cb * scale, sb * scale
        trig[0], trig[1] = unit_circle(wave * lane * 128.0)
        for q in range(LONS // 128):
            ca = trig[0, :, q : q + 1]
            sa = trig[1, :, q : q + 1]
            half32[pl.ds(0, 128, 2), :] = ca * cb - sa * sb
            half32[pl.ds(1, 128, 2), :] = -(sa * cb + ca * sb)
            tab[r, :, q * 128 : (q + 1) * 128] = half32[...].astype(BF16)
        if r == ROUNDS - 1:
            tab_copy().start()

    def by_row(r):
        return sent.at[r].reshape(ROWS, PEERS, 2, LANES)

    def by_level(r):
        return sent.at[r].reshape(LEV, DEGREES, 2, LANES)

    def forward(r, first, count):
        def pair(p, carry):
            if r == 0:

                @pl.when(p % 2 == 0)
                def _():
                    grid_copy(p // 2).wait()

            rows = gv.reshape(ROWS * LANES, LONS)[pl.ds(pl.multiple_of(p * 256, 256), 256), :]
            out = lax.dot_general(tab[r], rows, NT, preferred_element_type=F32).astype(BF16)
            for h in range(2):
                place = sent.at[r, pl.ds((2 * p + h) * PEERS, PEERS)]
                place.reshape(256, 128)[...] = out[:, h * 128 : (h + 1) * 128]
            return carry

        lax.fori_loop(first // 2, (first + count) // 2, pair, 0)

    def send_forward(r, first, count):
        def send(i2, j2):
            pltpu.make_async_remote_copy(
                src_ref=by_row(r).at[pl.ds(first, count), i2 * LEV + j2],
                dst_ref=frecv.at[r, j, pl.ds(i * ROWS + first, count)],
                send_sem=fsend_sem.at[r],
                recv_sem=frecv_sem.at[r],
                device_id=(i2, j2),
                device_id_type=MESH,
            ).start()

        to_partners(send)
        frecv[r, j, pl.ds(i * ROWS + first, count)] = by_row(r)[first : first + count, me]

    def send_back(r):
        def send(i2, j2):
            pltpu.make_async_remote_copy(
                src_ref=by_level(r).at[j2, pl.ds(i2 * ROWS, ROWS)],
                dst_ref=landing(r).at[:, me],
                send_sem=bsend_sem.at[r],
                recv_sem=brecv_sem.at[r],
                device_id=(i2, j2),
                device_id_type=MESH,
            ).start()

        to_partners(send)
        if r < ROUNDS - 1:
            brecv[r, :, me] = by_level(r)[j, pl.ds(i * ROWS, ROWS)]
        else:
            own_copy().start()

    def own_copy():
        return pltpu.make_async_copy(
            by_level(ROUNDS - 1).at[j, pl.ds(i * ROWS, ROWS)], last.at[:, me], own_sem
        )

    def part_copy(s):
        return pltpu.make_async_copy(
            part.at[s % 2], part_out.at[pl.ds(s * CHUNK * 128, CHUNK * 128)], part_sem.at[s % 2]
        )

    def wait_bytes(ref, r, sem):
        most = ref.reshape(ROWS * PEERS, 2, LANES).at[pl.ds(0, ROWS * (PEERS - 1))]
        pltpu.make_async_copy(most, most, sem.at[r]).wait()

    def level_copy(src, dst, s, d):
        return pltpu.make_async_remote_copy(
            src_ref=src,
            dst_ref=dst.at[j],
            send_sem=vsend_sem.at[s],
            recv_sem=vrecv_sem.at[s],
            device_id=(i, (j + d) % LEV),
            device_id_type=MESH,
        )

    def build_mixer():
        for s, ref in enumerate((vertx, dampx)):
            three = ref.at[pl.ds(0, LEV - 1)]
            pltpu.make_async_copy(three, three, vrecv_sem.at[s]).wait()
            pltpu.make_async_copy(three, three, vsend_sem.at[s]).wait()
        for p in range(LEV):
            vfull[p * 32 : (p + 1) * 32, :] = vertx[p]
        row = lax.broadcasted_iota(jnp.int32, (512, 128), 0)
        col = lax.broadcasted_iota(jnp.int32, (512, 128), 1)
        pick = jnp.where(row // 4 == col, 1.0, 0.0).astype(BF16)
        tall = lax.dot_general(pick, vfull[...], NT, preferred_element_type=F32).astype(BF16)
        wide = lax.dot_general(tall, pick, NT, preferred_element_type=F32)
        row = lax.broadcasted_iota(jnp.int32, (512, 512), 0)
        col = lax.broadcasted_iota(jnp.int32, (512, 512), 1)
        mixer[...] = jnp.where(row % 4 == col % 4, wide, 0.0).astype(BF16)
        near = jnp.where(row[:, 0:128] // 4 % 32 == col[:, 0:128], 1.0, 0.0).astype(BF16)
        lane = lax.broadcasted_iota(jnp.int32, (16, 512), 1)
        damp = jnp.zeros((16, 512), F32)
        for p in range(LEV):
            found = lax.dot_general(dampx[p], near, NT, preferred_element_type=F32)
            damp = damp + jnp.where(lane // 128 == p, found, 0.0)
        damp = damp[0:1, :]
        for t in range(ROUNDS):
            n = (lax.broadcasted_iota(jnp.int32, (128, 512), 0) + 128 * t).astype(F32)
            ratio = n * (n + 1.0) / float(DEGREES * (DEGREES - 1))
            factor[t * 128 : (t + 1) * 128, :] = 1.0 / (1.0 + damp * (ratio * ratio))

    def spectral(r):
        wave = wave_ref[me * ROUNDS + r]
        weight = jnp.where(wave == 0, 1.0, 2.0).astype(F32)
        for p in range(LEV):
            pair32[...] = frecv.at[r, p].reshape(2 * DEGREES, 128)[...].astype(F32)
            for h in range(2):
                xr[:, h * 512 + p * 128 : h * 512 + (p + 1) * 128] = pair32[
                    pl.ds(h, DEGREES, 2), :
                ].astype(BF16)
        keep = jnp.where(2 * wave < lon_ref[...], 1.0, 0.0).reshape(1, DEGREES)
        for t in range(r, ROUNDS):
            n = lax.broadcasted_iota(jnp.int32, (128, DEGREES), 0) + 128 * t
            tile = jnp.where(n >= wave, legv[r, t * 128 : (t + 1) * 128, :].astype(F32), 0.0)
            tile = (tile * keep).astype(BF16)
            legm[t * 128 : (t + 1) * 128, :] = tile
            spec = jnp.dot(tile, xr[...], preferred_element_type=F32).astype(BF16)
            for h in range(2):
                part = spec[:, h * 512 : (h + 1) * 512]
                total = part.astype(F32) + jnp.dot(
                    part, mixer[...], preferred_element_type=F32
                )
                total = total * factor[t * 128 : (t + 1) * 128, :] * weight
                mixed[t * 128 : (t + 1) * 128, h * 512 : (h + 1) * 512] = total.astype(BF16)
        for s in range(ROUNDS):
            out = lax.dot_general(
                legm[r * 128 :, s * 128 : (s + 1) * 128],
                mixed[r * 128 :, :],
                TN,
                preferred_element_type=F32,
            )
            for p in range(LEV):
                for h in range(2):
                    half32[pl.ds(h, 128, 2), :] = out[
                        :, h * 512 + p * 128 : h * 512 + (p + 1) * 128
                    ]
                place = sent.at[r, pl.ds(p * DEGREES + s * 128, 128)]
                place.reshape(256, 128)[...] = half32[...].astype(BF16)

    small[0].wait()
    table(0)
    forward(0, 0, 8)
    pl.semaphore_wait(barrier, PEERS - 1)
    send_forward(0, 0, 8)
    forward(0, 8, 12)
    send_forward(0, 8, 12)
    for copy in small[1:]:
        copy.start()
    for r in range(ROUNDS):
        leg_copy(r).start()
    for copy in small[1:]:
        copy.wait()
    damp16[...] = jnp.zeros_like(damp16)
    damp16[:, 0:32] = jnp.broadcast_to(damp_ref[...].astype(F32).reshape(1, 32), (16, 32)).astype(
        BF16
    )
    for d in range(1, LEV):
        level_copy(vert_ref, vertx, 0, d).start()
        level_copy(damp16, dampx, 1, d).start()
    dampx[j] = damp16[...]
    for r in range(1, ROUNDS):
        table(r)
        forward(r, 0, ROWS)
        send_forward(r, 0, ROWS)
    build_mixer()
    for r in range(ROUNDS):
        leg_copy(r).wait()
        wait_bytes(sent.at[r], r, fsend_sem)
        wait_bytes(frecv.at[r], r, frecv_sem)
        spectral(r)
        send_back(r)
    for r in range(ROUNDS - 1):
        wait_bytes(brecv.at[r], r, brecv_sem)
    for s in range(ROWS // CHUNK):
        for a in range(CHUNK):
            for r in range(ROUNDS - 1):
                block = brecv.at[r, s * CHUNK + a].reshape(256, 128)[...]
                lhs[a * 128 : (a + 1) * 128, r * 256 : (r + 1) * 256] = block.T
        if s >= 2:
            part_copy(s - 2).wait()
        part[s % 2] = jnp.dot(
            lhs[...],
            tab[0 : ROUNDS - 1].reshape((ROUNDS - 1) * 256, LONS),
            preferred_element_type=F32,
        ).astype(BF16)
        part_copy(s).start()
    for s in range(ROWS // CHUNK - 2, ROWS // CHUNK):
        part_copy(s).wait()
    tab_copy().wait()
    for r in range(ROUNDS):
        wait_bytes(sent.at[r], r, bsend_sem)
    own_copy().wait()
    wait_bytes(last, ROUNDS - 1, brecv_sem)


def hops(q):
    return sum(min(d, 4 - d) for d in (q // 32, q // 8 % 4, q % 4))


def unit_circle(steps):
    turns = jnp.floor(steps * (1.0 / LONS))
    rest = steps - turns * LONS
    rest = jnp.where(rest < 0.0, rest + LONS, rest)
    rest = jnp.where(rest >= LONS, rest - LONS, rest)
    quarter = jnp.floor(rest * (4.0 / LONS) + 0.5)
    y = (rest - quarter * (LONS // 4)) * (2.0 * math.pi / LONS)
    y2 = y * y
    sine = y * (1 + y2 * (-1 / 6 + y2 * (1 / 120 + y2 * (-1 / 5040 + y2 * (1 / 362880)))))
    cosine = 1 + y2 * (
        -1 / 2 + y2 * (1 / 24 + y2 * (-1 / 720 + y2 * (1 / 40320 - y2 * (1 / 3628800))))
    )
    odd = (quarter == 1.0) | (quarter == 3.0)
    first = jnp.where(odd, sine, cosine)
    second = jnp.where(odd, cosine, sine)
    back = (quarter == 2.0) | (quarter == 3.0)
    left = (quarter == 1.0) | (quarter == 2.0)
    return jnp.where(left, -first, first), jnp.where(back, -second, second)


def step(grid, legendre, vertical, damp, lon, waves):
    dma = pltpu.SemaphoreType.DMA
    any_spec = pl.BlockSpec(memory_space=pl.ANY)
    return pl.pallas_call(
        step_kernel,
        out_shape=(
            jax.ShapeDtypeStruct((ROWS, PEERS, 2, LANES), BF16),
            jax.ShapeDtypeStruct((ROWS * LANES, LONS), BF16),
            jax.ShapeDtypeStruct((256, LONS), BF16),
        ),
        in_specs=[pl.BlockSpec(memory_space=pltpu.HBM)] * 6,
        out_specs=(any_spec, any_spec, any_spec),
        scratch_shapes=[
            pltpu.VMEM((ROWS // CHUNK, CHUNK * LANES, LONS), BF16),
            pltpu.VMEM((ROUNDS, DEGREES, DEGREES), BF16),
            pltpu.VMEM((ROUNDS, 256, LONS), BF16),
            pltpu.VMEM((ROUNDS, ROWS * PEERS, 2, LANES), BF16),
            pltpu.VMEM((ROUNDS, LEV, DEGREES, 2, LANES), BF16),
            pltpu.VMEM((ROUNDS - 1, ROWS, PEERS, 2, LANES), BF16),
            pltpu.VMEM((LEV, 32, 128), BF16),
            pltpu.VMEM((LEV, 16, 128), BF16),
            pltpu.VMEM((16, 128), BF16),
            pltpu.VMEM((128, 128), BF16),
            pltpu.VMEM((512, 512), BF16),
            pltpu.VMEM((DEGREES, 512), F32),
            pltpu.SMEM((DEGREES,), jnp.int32),
            pltpu.VMEM((DEGREES,), jnp.int32),
            pltpu.VMEM((32,), BF16),
            pltpu.VMEM((PEERS, 128), jnp.int32),
            pltpu.VMEM((2, PEERS, 128), F32),
            pltpu.VMEM((2 * DEGREES, 128), F32),
            pltpu.VMEM((256, 128), F32),
            pltpu.VMEM((DEGREES, 1024), BF16),
            pltpu.VMEM((DEGREES, DEGREES), BF16),
            pltpu.VMEM((DEGREES, 1024), BF16),
            pltpu.VMEM((CHUNK * 128, (ROUNDS - 1) * 256), BF16),
            pltpu.VMEM((2, CHUNK * 128, LONS), BF16),
            dma((ROWS // CHUNK,)), dma((ROUNDS,)), dma, dma((2,)), dma((2,)),
            dma((ROUNDS,)), dma((ROUNDS,)), dma((ROUNDS,)), dma((ROUNDS,)), dma, dma((2,)), dma((4,)),
        ],
        compiler_params=pltpu.CompilerParams(
            collective_id=0, has_side_effects=True, vmem_limit_bytes=67043328
        ),
    )(grid, legendre, vertical, damp, lon, waves)


def finish_kernel(last_ref, tab_ref, part_ref, out_ref, stage, sem):
    s = pl.program_id(0)
    slot = s % 2

    def out_copy(step, where):
        return pltpu.make_async_copy(
            stage.at[where],
            out_ref.at[pl.ds(step * PIECE, PIECE)].reshape(PIECE * LANES, LONS),
            sem.at[where],
        )

    @pl.when(s >= 2)
    def _():
        out_copy(s - 2, slot).wait()

    for a in range(PIECE):
        block = last_ref.at[a].reshape(256, 128)[...]
        out = lax.dot_general(block, tab_ref[...], TN, preferred_element_type=F32)
        rows = slice(a * 128, (a + 1) * 128)
        stage[slot, rows, :] = (out + part_ref[rows, :].astype(F32)).astype(BF16)
    out_copy(s, slot).start()

    @pl.when(s == pl.num_programs(0) - 1)
    def _():
        out_copy(s - 1, 1 - slot).wait()
        out_copy(s, slot).wait()


def finish(last, part, tab):
    return pl.pallas_call(
        finish_kernel,
        grid=(ROWS // PIECE,),
        out_shape=jax.ShapeDtypeStruct((ROWS, 32, 4, LONS), BF16),
        in_specs=[
            pl.BlockSpec((PIECE, PEERS, 2, LANES), lambda s: (s, 0, 0, 0)),
            pl.BlockSpec((256, LONS), lambda s: (0, 0)),
            pl.BlockSpec((PIECE * 128, LONS), lambda s: (s, 0)),
        ],
        out_specs=pl.BlockSpec(memory_space=pl.ANY),
        scratch_shapes=[
            pltpu.VMEM((2, PIECE * 128, LONS), BF16),
            pltpu.SemaphoreType.DMA((2,)),
        ],
        compiler_params=pltpu.CompilerParams(vmem_limit_bytes=62 * 2**20),
    )(last, tab, part)


def per_device(grid, legendre, vertical, damping, lon_counts, wave_slots):
    last, part, tab = step(grid, legendre, vertical, damping, lon_counts, wave_slots)
    return finish(last, part, tab)


def solution(mesh):
    return jax.shard_map(
        per_device,
        mesh=mesh,
        in_specs=(
            P("lat", "lev", None, None),
            P("lat", None, None),
            P("lev", None),
            P("lev"),
            P(),
            P(),
        ),
        out_specs=P("lat", "lev", None, None),
        check_vma=False,
    )
```
